512 devices in a mesh: grp: 32 (over z, core), dev: 16 (over y, x).
Axes of the slice: x: 4, y: 4, z: 16, core: 2. Of those that a mesh axis runs over, the one named last changes fastest.
Arguments:
- sketch: float32 [524288, 512], P(('grp', 'dev')), may hold values from -50 to 50
- row_counts: int32 [512], P(('grp', 'dev')), may hold values from 0 to 1024, as said below
Outputs:
- q_factor: float32 [524288, 512], P(('grp', 'dev'))
- r_factor: float32 [512, 512], P('dev')
The draws below stay inside these ranges and needn't reach their ends.
Inputs may be any that keep to these rules, and one draw needn't show every extreme that they name: `row_counts`: every entry is a multiple of 128. Each aligned group of 16 consecutive entries sums to 4096, and in each such group at least one entry equals 1024.
All inputs are finite; a program needn't handle non-finite values.
Results may differ from the reference program's by a relative error of at most 0.00015.
Values sent between devices are 32-bit elements; how exact they have to be, the bound alone decides.
No kernel may reach another device: no remote copies, remote signals or barrier semaphores. Data moves between devices by JAX's collectives and lax.ppermute only.
A program may use at most 128 MiB of HBM per device.

```python
import math
import jax
import jax.numpy as jnp
from jax import lax

W = 512
BLOCK = 64
SLOTS = 16
HOLD = 4
CAP = 1024
ROWS = 524288
USED = 131072
N_GRP = 32
N_DEV = 16
DEVICES = 512


def units_of_group(group_key):
    units_max = SLOTS // 2
    units_total = N_DEV * HOLD // 2
    key_heavy, key_order = jax.random.split(group_key)
    heavy = jax.random.randint(key_heavy, (), 0, N_DEV)
    ordering = jax.random.permutation(key_order, (N_DEV - 1) * units_max)
    chosen = ordering[:units_total - units_max] // units_max
    others = jnp.sum((chosen[:, None] == jnp.arange(N_DEV - 1)[None, :]).astype(jnp.int32), axis=0)
    members = jnp.arange(N_DEV)
    other_place = jnp.clip(members - (members > heavy).astype(jnp.int32), 0, N_DEV - 2)
    return jnp.where(members == heavy, units_max, others[other_place])


def draw_row_counts(key, part):
    group_keys = jax.random.split(jax.random.fold_in(key, 11), N_GRP)
    units = jax.vmap(units_of_group)(group_keys).reshape(-1)
    return (units * (2 * BLOCK)).astype(jnp.int32)


def pair_columns(values, pair_key, lowest, highest):
    key_order, key_weight = jax.random.split(pair_key)
    ordering = jax.random.permutation(key_order, W)
    pair_count = W // 8
    leading = ordering[:pair_count]
    trailing = ordering[pair_count:2 * pair_count]
    weights = jnp.exp(jax.random.uniform(key_weight, (pair_count,), jnp.float32, math.log(lowest), math.log(highest)))
    nearby = values[:, leading] + weights[None, :] * values[:, trailing]
    return values.at[:, trailing].set(nearby)


def device_rise(rise):
    place = (jnp.arange(ROWS, dtype=jnp.int32) // CAP).astype(jnp.float32) / max(DEVICES - 1, 1)
    return jnp.exp(math.log(rise) * place)[:, None]


def draw_sketch(key, part):
    keys = jax.random.split(jax.random.fold_in(key, 23), 6)
    values = jax.random.truncated_normal(keys[0], -6.0, 6.0, (ROWS, W), jnp.float32)
    return (device_rise(3.0) * pair_columns(values, keys[5], 0.2, 0.5)).astype(jnp.float32)


def setup_inputs(seed: int = 0) -> dict:
    streams_of = jax.random.split(jax.random.key(seed), 3)
    return {
        "sketch": draw_sketch(jax.random.fold_in(streams_of[2], 71), 0),
        "row_counts": draw_row_counts(jax.random.fold_in(streams_of[2], 71), 0),
    }


def reference(sketch, row_counts):
    shaped = sketch.reshape(DEVICES, SLOTS * BLOCK, W)
    inside = jnp.arange(SLOTS * BLOCK, dtype=jnp.int32)[None, :] < row_counts[:, None]
    masked = jnp.where(inside[:, :, None], shaped, jnp.zeros((), sketch.dtype)).reshape(-1, W)
    gram_sum = lax.dot_general(masked, masked, (((0,), (0,)), ((), ())), precision=lax.Precision.HIGHEST) / USED
    upper_factor = jnp.linalg.cholesky(gram_sum).T
    orthonormal = lax.linalg.triangular_solve(upper_factor, masked, left_side=False, lower=False)
    return (orthonormal, upper_factor)
```

```python
import functools

import jax
import jax.numpy as jnp
from jax import lax
from jax.experimental import pallas as pl
from jax.experimental.pallas import tpu as pltpu
from jax.sharding import Mesh
from jax.sharding import PartitionSpec as P

SLOTS = 16
HOLD = 4
B = 128
NB = 32
SUB = 8
DEV = ("y", "x")
ALL = ("z", "core", "y", "x")
HIGH = lax.Precision.HIGHEST
WHOLE = pl.BlockSpec(memory_space=pltpu.VMEM)


def dot(left, right, dims=((1,), (0,))):
    return lax.dot_general(
        left, right, (dims, ((), ())), precision=HIGH, preferred_element_type=jnp.float32
    )


def upper_blocks(order):
    count = order // B
    return [(i, j) for i in range(count) for j in range(i, count)]


def gram_kernel(count_ref, rows_ref, packed_ref):
    capacity, order = rows_ref.shape
    row = lax.broadcasted_iota(jnp.int32, (capacity, order), 0)
    live = jnp.where(row < count_ref[0], rows_ref[...], 0.0)
    at = 0
    for i in range(order // B):
        wide = dot(live[:, i * B : (i + 1) * B], live[:, i * B :], ((0,), (0,)))
        for j in range(order // B - i):
            packed_ref[at : at + B, :] = wide[:, j * B : (j + 1) * B]
            at += B


def gram_of(rows_in, count):
    order = rows_in.shape[1]
    return pl.pallas_call(
        gram_kernel,
        out_shape=jax.ShapeDtypeStruct((len(upper_blocks(order)) * B, B), jnp.float32),
        in_specs=[pl.BlockSpec(memory_space=pltpu.SMEM), WHOLE],
        out_specs=WHOLE,
        name="gram",
    )(count, rows_in)


def spread(row):
    return jnp.broadcast_to(row, (SUB, row.shape[1]))


def eliminate(strip, at):
    groups = NB // SUB
    lane = lax.broadcasted_iota(jnp.int32, (SUB, B), 1)
    sub = lax.broadcasted_iota(jnp.int32, (SUB, B), 0)
    raw = [strip[v * SUB : (v + 1) * SUB] for v in range(groups)]
    diagonal = (lane >= at) & (lane < at + NB)
    aug = [
        jnp.where(diagonal, (lane == sub + (at + v * SUB)).astype(jnp.float32), raw[v])
        for v in range(groups)
    ]
    cols = [
        [
            None
            if v < j // SUB
            else jnp.broadcast_to(raw[v][:, at + j : at + j + 1], (SUB, B))
            for v in range(groups)
        ]
        for j in range(NB)
    ]
    for j in range(NB):
        first, r = divmod(j, SUB)
        root = lax.rsqrt(spread(cols[j][first][r : r + 1]))
        scaled = [None if c is None else c * root for c in cols[j]]
        row_raw = spread(raw[first][r : r + 1]) * root
        row_aug = spread(aug[first][r : r + 1]) * root
        below = jnp.where(sub > r, scaled[first], 0.0)
        raw[first] = jnp.where(sub == r, row_raw, raw[first] - below * row_raw)
        aug[first] = jnp.where(sub == r, row_aug, aug[first] - below * row_aug)
        for v in range(first + 1, groups):
            raw[v] = raw[v] - scaled[v] * row_raw
            aug[v] = aug[v] - scaled[v] * row_aug
        for l in range(j + 1, NB):
            g, q = divmod(l, SUB)
            factor = spread(scaled[g][q : q + 1])
            for v in range(g, groups):
                cols[l][v] = cols[l][v] - scaled[v] * factor
        cols[j] = None
    return jnp.concatenate(raw), jnp.concatenate(aug)


def factor_block(block):
    strips = [block[b * NB : (b + 1) * NB] for b in range(B // NB)]
    lane = lax.broadcasted_iota(jnp.int32, (NB, B), 1)
    sub = lax.broadcasted_iota(jnp.int32, (NB, B), 0)
    upper, inverse = [], []
    for b in range(B // NB):
        at = b * NB
        raw, aug = eliminate(strips[b], at)
        upper.append(jnp.where(lane >= sub + at, raw, 0.0))
        inverse.append(jnp.where(lane <= sub + at, aug, 0.0))
        if at + NB < B:
            change = dot(raw.T[at + NB :], aug)
            hit = (lane >= at) & (lane < at + NB)
            for i in range(b + 1, B // NB):
                o = (i - b - 1) * NB
                strips[i] = jnp.where(hit, 0.0, strips[i]) - change[o : o + NB]
    return jnp.concatenate(upper), jnp.concatenate(inverse)


def factor_kernel(scale, packed_ref, upper_ref, inverse_ref, work):
    order = work.shape[0]
    for p, (i, j) in enumerate(upper_blocks(order)):
        work[i * B : (i + 1) * B, j * B : (j + 1) * B] = (
            packed_ref[p * B : (p + 1) * B, :] * scale
        )
    for s in range(order // B):
        lo, hi = s * B, (s + 1) * B
        here = slice(lo, hi)
        upper, inverse = factor_block(work[here, here])
        upper_ref[here, here] = upper
        inverse_ref[here, here] = inverse
        parts = []
        if lo:
            left = dot(inverse, work[here, :lo])
            inverse_ref[here, :lo] = left
            upper_ref[here, :lo] = jnp.zeros((B, lo), jnp.float32)
            parts.append(left)
        parts.append(inverse)
        if hi < order:
            right = dot(inverse, work[here, hi:])
            upper_ref[here, hi:] = right
            inverse_ref[here, hi:] = jnp.zeros((B, order - hi), jnp.float32)
            parts.append(right)
            change = dot(right.T, jnp.concatenate(parts, axis=1))
            if lo:
                work[hi:, :lo] = work[hi:, :lo] - change[:, :lo]
            work[hi:, here] = -change[:, here]
            work[hi:, hi:] = work[hi:, hi:] - change[:, hi:]


def factors_of(packed, order, scale):
    return pl.pallas_call(
        functools.partial(factor_kernel, scale),
        out_shape=[jax.ShapeDtypeStruct((order, order), jnp.float32)] * 2,
        in_specs=[WHOLE],
        out_specs=[WHOLE] * 2,
        scratch_shapes=[pltpu.VMEM((order, order), jnp.float32)],
        name="factor",
    )(packed)


def apply_kernel(count_ref, rows_ref, inverse_ref, out_ref):
    height, order = rows_ref.shape
    row = lax.broadcasted_iota(jnp.int32, (height, order), 0)
    start = pl.program_id(0) * height
    live = jnp.where(row + start < count_ref[0], rows_ref[...], 0.0)
    half = order // 2
    for k in range(2):
        hi = (k + 1) * half
        out_ref[:, k * half : hi] = dot(
            live[:, :hi], inverse_ref[k * half : hi, :hi], ((1,), (1,))
        )


def applied(rows_in, count, inverse):
    capacity, order = rows_in.shape
    height = capacity // 4
    tile = pl.BlockSpec((height, order), lambda i: (i, 0))
    return pl.pallas_call(
        apply_kernel,
        grid=(capacity // height,),
        out_shape=jax.ShapeDtypeStruct(rows_in.shape, jnp.float32),
        in_specs=[
            pl.BlockSpec(memory_space=pltpu.SMEM),
            tile,
            pl.BlockSpec((order, order), lambda i: (0, 0)),
        ],
        out_specs=tile,
        name="apply",
    )(count, rows_in, inverse)


def everyone(value, axis):
    copies = jnp.broadcast_to(value, (lax.axis_size(axis), *value.shape))
    return lax.all_to_all(copies, axis, split_axis=0, concat_axis=0, tiled=True)


def swapped(value):
    return lax.ppermute(value, "core", [(0, 1), (1, 0)])


def summed(packed):
    members = lax.axis_size(DEV)
    tiles = packed.reshape(members, -1, B)
    own = lax.all_to_all(tiles, DEV, split_axis=0, concat_axis=0, tiled=True).sum(axis=0)
    core = lax.axis_index("core")
    half = own.shape[0] // 2
    mine = lax.dynamic_slice_in_dim(own, core * half, half, 0)
    other = lax.dynamic_slice_in_dim(own, (1 - core) * half, half, 0)
    part = everyone(mine + swapped(other), "z").sum(axis=0)
    back = swapped(part)
    own = jnp.where(core == 0, jnp.stack([part, back]), jnp.stack([back, part]))
    return everyone(own.reshape(-1, B), DEV).reshape(-1, B)


def shards(sketch, row_counts):
    capacity, order = sketch.shape
    members = lax.axis_size(DEV)
    row_total = lax.axis_size(ALL) * HOLD * (capacity // SLOTS)
    packed = summed(gram_of(sketch, row_counts))
    upper, inverse = factors_of(packed, order, 1.0 / row_total)
    share = order // members
    r_rows = lax.dynamic_slice_in_dim(upper, lax.axis_index(DEV) * share, share, 0)
    return (applied(sketch, row_counts, inverse), r_rows)


def solution(mesh):
    finer = Mesh(mesh.devices.reshape(16, 2, 4, 4), ALL)
    return jax.shard_map(
        shards,
        mesh=finer,
        in_specs=(P(ALL, None), P(ALL)),
        out_specs=(P(ALL, None), P(DEV, None)),
        check_vma=False,
    )
```

```python
import functools

import jax
import jax.numpy as jnp
from jax import lax
from jax.experimental import pallas as pl
from jax.experimental.pallas import tpu as pltpu
from jax.sharding import Mesh
from jax.sharding import PartitionSpec as P

SLOTS = 16
HOLD = 4
B = 128
NB = 32
SUB = 8
CHUNKS = 4
ROOM = 24 * 1024 * 1024
MOST = 65_600_000
DEV = ("y", "x")
ALL = ("z_high", "z_low", "core", "y", "x")
PLANE = ("core", "y", "x")
HIGH = lax.Precision.HIGHEST
WHOLE = pl.BlockSpec(memory_space=pltpu.VMEM)
FAR = pl.BlockSpec(memory_space=pltpu.HBM)


def dot(left, right, dims=((1,), (0,))):
    return lax.dot_general(
        left, right, (dims, ((), ())), precision=HIGH, preferred_element_type=jnp.float32
    )


def upper_blocks(order):
    count = order // B
    return [(i, j) for i in range(count) for j in range(i, count)]


def halves(value):
    top = value.astype(jnp.bfloat16)
    return top, (value - top.astype(jnp.float32)).astype(jnp.bfloat16)


def narrow_dot(left, right, dims=((1,), (0,))):
    return lax.dot_general(left, right, (dims, ((), ())), preferred_element_type=jnp.float32)


def gram_kernel(count_ref, rows_ref, packed_ref, rows, sems):
    capacity, order = rows.shape
    height = capacity // CHUNKS
    wide = order // 2
    copies = [
        pltpu.make_async_copy(
            rows_ref.at[pl.ds(c * height, height)],
            rows.at[pl.ds(c * height, height)],
            sems.at[c],
        )
        for c in range(CHUNKS)
    ]
    for copy in copies:
        copy.start()
    row = lax.broadcasted_iota(jnp.int32, (height, order), 0)
    totals = None
    for c in range(CHUNKS):
        copies[c].wait()
        live = jnp.where(
            row < count_ref[0] - c * height, rows[c * height : (c + 1) * height, :], 0.0
        )
        top, low = halves(live)
        top_t, low_t = halves(live.T)
        terms = []
        for lhs_rows, columns in ((wide, slice(0, wide)), (order, slice(wide, order))):
            term = narrow_dot(top_t[:lhs_rows], top[:, columns])
            term += narrow_dot(low_t[:lhs_rows], top[:, columns])
            term += narrow_dot(top_t[:lhs_rows], low[:, columns])
            term += narrow_dot(low_t[:lhs_rows], low[:, columns])
            terms.append(term)
        totals = terms if totals is None else [t + u for t, u in zip(totals, terms)]
    for p, (i, j) in enumerate(upper_blocks(order)):
        side, inner = divmod(j * B, wide)
        packed_ref[p * B : (p + 1) * B, :] = totals[side][i * B : (i + 1) * B, inner : inner + B]


def gram_of(rows_in, count):
    capacity, order = rows_in.shape
    return pl.pallas_call(
        gram_kernel,
        out_shape=jax.ShapeDtypeStruct((len(upper_blocks(order)) * B, B), jnp.float32),
        in_specs=[pl.BlockSpec(memory_space=pltpu.SMEM), FAR],
        out_specs=WHOLE,
        scratch_shapes=[
            pltpu.VMEM((capacity, order), jnp.float32),
            pltpu.SemaphoreType.DMA((CHUNKS,)),
        ],
        compiler_params=pltpu.CompilerParams(vmem_limit_bytes=MOST),
        name="gram",
    )(count, rows_in)


def spread(row):
    return jnp.broadcast_to(row, (SUB, row.shape[1]))


def eliminate(strip, at):
    groups = NB // SUB
    lane = lax.broadcasted_iota(jnp.int32, (SUB, B), 1)
    sub = lax.broadcasted_iota(jnp.int32, (SUB, B), 0)
    raw = [strip[v * SUB : (v + 1) * SUB] for v in range(groups)]
    diagonal = (lane >= at) & (lane < at + NB)
    aug = [
        jnp.where(diagonal, (lane == sub + (at + v * SUB)).astype(jnp.float32), raw[v])
        for v in range(groups)
    ]
    cols = [
        [
            None
            if v < j // SUB
            else jnp.broadcast_to(raw[v][:, at + j : at + j + 1], (SUB, B))
            for v in range(groups)
        ]
        for j in range(NB)
    ]
    for j in range(NB):
        first, r = divmod(j, SUB)
        root = lax.rsqrt(spread(cols[j][first][r : r + 1]))
        scaled = [None if c is None else c * root for c in cols[j]]
        row_raw = spread(raw[first][r : r + 1]) * root
        row_aug = spread(aug[first][r : r + 1]) * root
        below = jnp.where(sub > r, scaled[first], 0.0)
        raw[first] = jnp.where(sub == r, row_raw, raw[first] - below * row_raw)
        aug[first] = jnp.where(sub == r, row_aug, aug[first] - below * row_aug)
        for v in range(first + 1, groups):
            raw[v] = raw[v] - scaled[v] * row_raw
            aug[v] = aug[v] - scaled[v] * row_aug
        for l in range(j + 1, NB):
            g, q = divmod(l, SUB)
            factor = spread(scaled[g][q : q + 1])
            for v in range(g, groups):
                cols[l][v] = cols[l][v] - scaled[v] * factor
        cols[j] = None
    return jnp.concatenate(raw), jnp.concatenate(aug)


def factor_block(block):
    strips = [block[b * NB : (b + 1) * NB] for b in range(B // NB)]
    lane = lax.broadcasted_iota(jnp.int32, (NB, B), 1)
    sub = lax.broadcasted_iota(jnp.int32, (NB, B), 0)
    upper, inverse = [], []
    for b in range(B // NB):
        at = b * NB
        raw, aug = eliminate(strips[b], at)
        upper.append(jnp.where(lane >= sub + at, raw, 0.0))
        inverse.append(jnp.where(lane <= sub + at, aug, 0.0))
        if at + NB < B:
            change = dot(raw.T[at + NB :], aug)
            hit = (lane >= at) & (lane < at + NB)
            for i in range(b + 1, B // NB):
                o = (i - b - 1) * NB
                strips[i] = jnp.where(hit, 0.0, strips[i]) - change[o : o + NB]
    return jnp.concatenate(upper), jnp.concatenate(inverse)


def factor(scale, packed_ref, upper_ref, inverse_ref, work):
    order = work.shape[0]
    for p, (i, j) in enumerate(upper_blocks(order)):
        work[i * B : (i + 1) * B, j * B : (j + 1) * B] = (
            packed_ref[p * B : (p + 1) * B, :] * scale
        )
    for s in range(order // B):
        lo, hi = s * B, (s + 1) * B
        here = slice(lo, hi)
        upper, inverse = factor_block(work[here, here])
        upper_ref[here, here] = upper
        inverse_ref[here, here] = inverse
        parts = []
        if lo:
            left = dot(inverse, work[here, :lo])
            inverse_ref[here, :lo] = left
            upper_ref[here, :lo] = jnp.zeros((B, lo), jnp.float32)
            parts.append(left)
        parts.append(inverse)
        if hi < order:
            right = dot(inverse, work[here, hi:])
            upper_ref[here, hi:] = right
            inverse_ref[here, hi:] = jnp.zeros((B, order - hi), jnp.float32)
            parts.append(right)
            change = dot(right.T, jnp.concatenate(parts, axis=1))
            if lo:
                work[hi:, :lo] = work[hi:, :lo] - change[:, :lo]
            work[hi:, here] = -change[:, here]
            work[hi:, hi:] = work[hi:, hi:] - change[:, hi:]


def solve_kernel(
    scale, scalars_ref, packed_ref, rows, out_ref, share_ref,
    work, upper, inverse, result, out_sems,
):
    capacity, order = rows.shape
    height = capacity // CHUNKS
    half = order // 2
    factor(scale, packed_ref, upper, inverse, work)
    share = share_ref.shape[0]
    at = pl.multiple_of(scalars_ref[1] * share, share)
    share_ref[...] = upper[pl.ds(at, share), :]
    top, low = halves(inverse[...])
    row = lax.broadcasted_iota(jnp.int32, (height, order), 0)
    stores = []
    for c in range(CHUNKS):
        span = slice(c * height, (c + 1) * height)
        live = jnp.where(row < scalars_ref[0] - c * height, rows[span, :], 0.0)
        live_top, live_low = halves(live)
        for k in range(2):
            lo, hi = k * half, (k + 1) * half
            value = narrow_dot(live_top[:, :hi], top[lo:hi, :hi], ((1,), (1,)))
            value += narrow_dot(live_low[:, :hi], top[lo:hi, :hi], ((1,), (1,)))
            value += narrow_dot(live_top[:, :hi], low[lo:hi, :hi], ((1,), (1,)))
            result[span, lo:hi] = value
        store = pltpu.make_async_copy(
            result.at[pl.ds(c * height, height)],
            out_ref.at[pl.ds(c * height, height)],
            out_sems.at[c],
        )
        store.start()
        stores.append(store)
    for store in stores:
        store.wait()


def solved(packed, rows_in, count, index, members, scale):
    capacity, order = rows_in.shape
    square = pltpu.VMEM((order, order), jnp.float32)
    tall = pltpu.VMEM((capacity, order), jnp.float32)
    return pl.pallas_call(
        functools.partial(solve_kernel, scale),
        out_shape=[
            jax.ShapeDtypeStruct(rows_in.shape, jnp.float32),
            jax.ShapeDtypeStruct((order // members, order), jnp.float32),
        ],
        in_specs=[pl.BlockSpec(memory_space=pltpu.SMEM), WHOLE, WHOLE],
        out_specs=[FAR, WHOLE],
        scratch_shapes=[
            square,
            square,
            square,
            tall,
            pltpu.SemaphoreType.DMA((CHUNKS,)),
        ],
        compiler_params=pltpu.CompilerParams(vmem_limit_bytes=ROOM),
        name="solve",
    )(jnp.stack([count[0], index]), packed, rows_in)


def exchanged(tiles, axis):
    return lax.all_to_all(tiles, axis, split_axis=0, concat_axis=0, tiled=True)


def everyone(value, axis):
    return exchanged(jnp.broadcast_to(value, (lax.axis_size(axis), *value.shape)), axis)


def summed(packed):
    tiles = packed.reshape(lax.axis_size(PLANE), -1, B)
    own = exchanged(tiles, PLANE).sum(axis=0)
    own = everyone(own, "z_low").sum(axis=0)
    own = everyone(own, "z_high").sum(axis=0)
    return everyone(own, PLANE).reshape(-1, B)


def shards(sketch, row_counts):
    capacity, order = sketch.shape
    members = lax.axis_size(DEV)
    row_total = lax.axis_size(ALL) * HOLD * (capacity // SLOTS)
    packed = summed(gram_of(sketch, row_counts))
    return solved(packed, sketch, row_counts, lax.axis_index(DEV), members, 1.0 / row_total)


def solution(mesh):
    finer = Mesh(mesh.devices.reshape(4, 4, 2, 4, 4), ALL)
    return jax.shard_map(
        shards,
        mesh=finer,
        in_specs=(P(ALL, None), P(ALL)),
        out_specs=(P(ALL, None), P(DEV, None)),
        check_vma=False,
    )
```

```python
import functools

import jax
import jax.numpy as jnp
from jax import lax
from jax.experimental import pallas as pl
from jax.experimental.pallas import tpu as pltpu
from jax.sharding import Mesh
from jax.sharding import PartitionSpec as P

SLOTS = 16
HOLD = 4
B = 128
NB = 32
SUB = 8
CHUNKS = 4
ROOM = 24 * 1024 * 1024
LEFT, RIGHT = (2, 1, 0, 1, 0, 0), (0, 1, 2, 0, 1, 0)
LEFT_WIDE, RIGHT_WIDE = (2, 1, *LEFT), (1, 2, *RIGHT)
DEV = ("y", "x")
ALL = ("z_high", "z_low", "core", "y", "x")
PLANE = ("core", "y", "x")
HIGH = lax.Precision.HIGHEST
WHOLE = pl.BlockSpec(memory_space=pltpu.VMEM)
FAR = pl.BlockSpec(memory_space=pltpu.HBM)


def dot(left, right, dims=((1,), (0,))):
    return lax.dot_general(
        left, right, (dims, ((), ())), precision=HIGH, preferred_element_type=jnp.float32
    )


def upper_blocks(order):
    count = order // B
    return [(i, j) for i in range(count) for j in range(i, count)]


def halves(value):
    top = value.astype(jnp.bfloat16)
    return top, (value - top.astype(jnp.float32)).astype(jnp.bfloat16)


def narrow_dot(left, right, dims=((1,), (0,))):
    return lax.dot_general(left, right, (dims, ((), ())), preferred_element_type=jnp.float32)


def gram_kernel(count_ref, rows, packed_ref, left_sum, right_sum):
    capacity, order = rows.shape
    height = capacity // CHUNKS
    wide = order // 2

    left_sum[...] = jnp.zeros_like(left_sum)
    right_sum[...] = jnp.zeros_like(right_sum)
    row = lax.broadcasted_iota(jnp.int32, (height, order), 0)

    @pl.loop(0, CHUNKS)
    def _(c):
        held = rows[pl.ds(pl.multiple_of(c * height, height), height), :]
        live = jnp.where(row < count_ref[0] - c * height, held, 0.0)
        top, low = halves(live)
        top_t, low_t = halves(live.T)
        for total, side in ((left_sum, slice(0, wide)), (right_sum, slice(wide, order))):
            tall = total.shape[0]
            term = narrow_dot(top_t[:tall], top[:, side])
            term += narrow_dot(low_t[:tall], top[:, side])
            term += narrow_dot(top_t[:tall], low[:, side])
            term += narrow_dot(low_t[:tall], low[:, side])
            total[...] += term

    for p, (i, j) in enumerate(upper_blocks(order)):
        side, inner = divmod(j * B, wide)
        total = (left_sum, right_sum)[side]
        packed_ref[p * B : (p + 1) * B, :] = total[i * B : (i + 1) * B, inner : inner + B]


def gram_of(rows_in, count):
    capacity, order = rows_in.shape
    return pl.pallas_call(
        gram_kernel,
        out_shape=jax.ShapeDtypeStruct((len(upper_blocks(order)) * B, B), jnp.float32),
        in_specs=[pl.BlockSpec(memory_space=pltpu.SMEM), WHOLE],
        out_specs=WHOLE,
        scratch_shapes=[
            pltpu.VMEM((order // 2, order // 2), jnp.float32),
            pltpu.VMEM((order, order // 2), jnp.float32),
        ],
        compiler_params=pltpu.CompilerParams(vmem_limit_bytes=ROOM),
        name="gram",
    )(count, rows_in)


def spread(row):
    return jnp.broadcast_to(row, (SUB, row.shape[1]))


def thirds(value):
    top = value.astype(jnp.bfloat16)
    rest = value - top.astype(jnp.float32)
    middle = rest.astype(jnp.bfloat16)
    return top, middle, (rest - middle.astype(jnp.float32)).astype(jnp.bfloat16)


def stacked(value, order, axis):
    parts = thirds(value)
    return jnp.concatenate([parts[k] for k in order], axis=axis)


def exact_dot(left, right):
    return narrow_dot(stacked(left, LEFT, 1), stacked(right, RIGHT, 0))


def eliminate(strip, at):
    groups = NB // SUB
    lane = lax.broadcasted_iota(jnp.int32, (SUB, B), 1)
    sub = lax.broadcasted_iota(jnp.int32, (SUB, B), 0)
    rows = [strip[v * SUB : (v + 1) * SUB] for v in range(groups)]
    cols = [
        [
            None
            if v < j // SUB
            else jnp.broadcast_to(rows[v][:, at + j : at + j + 1], (SUB, B))
            for v in range(groups)
        ]
        for j in range(NB)
    ]
    diagonal = (lane >= at) & (lane < at + NB)
    rows = [
        jnp.where(diagonal, (lane == sub + (at + v * SUB)).astype(jnp.float32), rows[v])
        for v in range(groups)
    ]
    done = list(rows)
    for j in range(NB):
        first, r = divmod(j, SUB)
        root = lax.rsqrt(spread(cols[j][first][r : r + 1]))
        scaled = [None if c is None else c * root for c in cols[j]]
        row = spread(rows[first][r : r + 1]) * root
        done[first] = jnp.where(sub == r, row, done[first])
        for l in range(j + 1, NB):
            g, q = divmod(l, SUB)
            factor = spread(scaled[g][q : q + 1])
            for v in range(g, groups):
                cols[l][v] = cols[l][v] - scaled[v] * factor
        for v in range(first, groups):
            rows[v] = rows[v] - scaled[v] * row
        cols[j] = None
    return jnp.concatenate(done)


def factor_block(block):
    strips = [block[b * NB : (b + 1) * NB] for b in range(B // NB)]
    lane = lax.broadcasted_iota(jnp.int32, (NB, B), 1)
    sub = lax.broadcasted_iota(jnp.int32, (NB, B), 0)
    inverse = []
    for b in range(B // NB):
        at = b * NB
        done = eliminate(strips[b], at)
        inverse.append(jnp.where(lane <= sub + at, done, 0.0))
        if at + NB < B:
            across = stacked(done, LEFT_WIDE, 0).T
            down = stacked(done, RIGHT_WIDE, 0)
            hit = (lane >= at) & (lane < at + NB)
            near = narrow_dot(across[at + NB : at + 2 * NB], down)
            strips[b + 1] = jnp.where(hit, 0.0, strips[b + 1]) - near
            if at + 2 * NB < B:
                rest = narrow_dot(across[at + 2 * NB :], down)
                for i in range(b + 2, B // NB):
                    o = (i - b - 2) * NB
                    strips[i] = jnp.where(hit, 0.0, strips[i]) - rest[o : o + NB]
    return jnp.concatenate(inverse)


def factor(scale, packed_ref, upper_ref, top_ref, low_ref, work):
    order = work.shape[0]
    for p, (i, j) in enumerate(upper_blocks(order)):
        work[i * B : (i + 1) * B, j * B : (j + 1) * B] = (
            packed_ref[p * B : (p + 1) * B, :] * scale
        )
    lane = lax.broadcasted_iota(jnp.int32, (B, B), 1)
    sub = lax.broadcasted_iota(jnp.int32, (B, B), 0)
    for s in range(order // B):
        lo, hi = s * B, (s + 1) * B
        here = slice(lo, hi)
        inverse = factor_block(work[here, here])
        across = stacked(inverse, LEFT, 1)
        if hi < order:
            near = slice(hi, hi + B)
            right = narrow_dot(across, stacked(work[here, near], RIGHT, 0))
            work[near, near] = work[near, near] - exact_dot(right.T, right)
            rights = [right]
            if hi + B < order:
                far = narrow_dot(across, stacked(work[here, hi + B :], RIGHT, 0))
                rights += [far[:, c : c + B] for c in range(0, far.shape[1], B)]
            for c, right in enumerate(rights):
                upper_ref[here, hi + c * B : hi + (c + 1) * B] = right
        own = narrow_dot(across, stacked(work[here, here], RIGHT, 0))
        upper_ref[here, here] = jnp.where(lane >= sub, own, 0.0)
        lefts = [inverse]
        if lo:
            left = narrow_dot(across, stacked(work[here, :lo], RIGHT, 0))
            upper_ref[here, :lo] = jnp.zeros((B, lo), jnp.float32)
            lefts = [left, inverse]
        lefts = jnp.concatenate(lefts, axis=1)
        top_ref[here, :hi], low_ref[here, :hi] = halves(lefts)
        if s % 2 == 0 and hi < order:
            top_ref[here, hi : hi + B] = jnp.zeros((B, B), jnp.bfloat16)
            low_ref[here, hi : hi + B] = jnp.zeros((B, B), jnp.bfloat16)
        if hi < order:
            turned = [stacked(right.T, LEFT, 1) for right in rights]
            change = narrow_dot(jnp.concatenate(turned), stacked(lefts, RIGHT, 0))
            if lo:
                work[hi:, :lo] = work[hi:, :lo] - change[:, :lo]
            work[hi:, here] = -change[:, lo:]
            for c in range(1, len(rights)):
                span = slice(hi + c * B, hi + (c + 1) * B)
                change = narrow_dot(
                    jnp.concatenate(turned[: c + 1]), stacked(rights[c], RIGHT, 0)
                )
                work[hi : hi + (c + 1) * B, span] = work[hi : hi + (c + 1) * B, span] - change


def solve_kernel(
    scale, scalars_ref, packed_ref, rows_ref, out_ref, share_ref,
    work, upper, top, low, result, sems,
):
    capacity, order = rows_ref.shape
    height = capacity // CHUNKS
    half = order // 2
    factor(scale, packed_ref, upper, top, low, work)
    share = share_ref.shape[0]
    share_ref[...] = upper[pl.ds(pl.multiple_of(scalars_ref[1] * share, share), share), :]
    row = lax.broadcasted_iota(jnp.int32, (height, order), 0)

    def store(c):
        span = pl.ds(pl.multiple_of(c * height, height), height)
        return pltpu.make_async_copy(result.at[span], out_ref.at[span], sems.at[c])

    @pl.loop(0, CHUNKS)
    def _(c):
        span = pl.ds(pl.multiple_of(c * height, height), height)
        live = jnp.where(row < scalars_ref[0] - c * height, rows_ref[span, :], 0.0)
        live_top, live_low = halves(live)
        for k in range(2):
            lo, hi = k * half, (k + 1) * half
            value = narrow_dot(live_top[:, :hi], top[lo:hi, :hi], ((1,), (1,)))
            value += narrow_dot(live_low[:, :hi], top[lo:hi, :hi], ((1,), (1,)))
            value += narrow_dot(live_top[:, :hi], low[lo:hi, :hi], ((1,), (1,)))
            result[span, lo:hi] = value
        store(c).start()

    for c in range(CHUNKS):
        store(c).wait()


def solved(packed, rows_in, scalars, members, scale):
    capacity, order = rows_in.shape
    square = pltpu.VMEM((order, order), jnp.float32)
    tall = pltpu.VMEM((capacity, order), jnp.float32)
    return pl.pallas_call(
        functools.partial(solve_kernel, scale),
        out_shape=[
            jax.ShapeDtypeStruct(rows_in.shape, jnp.float32),
            jax.ShapeDtypeStruct((order // members, order), jnp.float32),
        ],
        in_specs=[pl.BlockSpec(memory_space=pltpu.SMEM), WHOLE, WHOLE],
        out_specs=[FAR, WHOLE],
        scratch_shapes=[
            square,
            square,
            pltpu.VMEM((order, order), jnp.bfloat16),
            pltpu.VMEM((order, order), jnp.bfloat16),
            tall,
            pltpu.SemaphoreType.DMA((CHUNKS,)),
        ],
        compiler_params=pltpu.CompilerParams(vmem_limit_bytes=ROOM),
        name="solve",
    )(scalars, packed, rows_in)


def exchanged(tiles, axis):
    return lax.all_to_all(tiles, axis, split_axis=0, concat_axis=0, tiled=True)


def everyone(value, axis):
    return exchanged(jnp.broadcast_to(value, (lax.axis_size(axis), *value.shape)), axis)


def summed(packed):
    tiles = packed.reshape(lax.axis_size(PLANE), -1, B)
    own = exchanged(tiles, PLANE).sum(axis=0)
    own = everyone(own, "z_low").sum(axis=0)
    own = everyone(own, "z_high").sum(axis=0)
    return everyone(own, PLANE).reshape(-1, B)


def shards(sketch, row_counts):
    capacity, order = sketch.shape
    members = lax.axis_size(DEV)
    row_total = lax.axis_size(ALL) * HOLD * (capacity // SLOTS)
    scalars = jnp.stack([row_counts[0], lax.axis_index(DEV)])
    packed = summed(gram_of(sketch, scalars))
    return solved(packed, sketch, scalars, members, 1.0 / row_total)


def solution(mesh):
    finer = Mesh(mesh.devices.reshape(4, 4, 2, 4, 4), ALL)
    return jax.shard_map(
        shards,
        mesh=finer,
        in_specs=(P(ALL, None), P(ALL)),
        out_specs=(P(ALL, None), P(DEV, None)),
        check_vma=False,
    )
```

```python
import functools

import jax
import jax.numpy as jnp
from jax import lax
from jax.experimental import pallas as pl
from jax.experimental.pallas import tpu as pltpu
from jax.sharding import Mesh
from jax.sharding import PartitionSpec as P

SLOTS = 16
HOLD = 4
B = 128
NB = 32
SUB = 8
CHUNKS = 4
ROOM = 24 * 1024 * 1024
LEFT, RIGHT = (2, 1, 0, 1, 0, 0), (0, 1, 2, 0, 1, 0)
LEFT_WIDE, RIGHT_WIDE = (2, 1, *LEFT), (1, 2, *RIGHT)
DEV = ("y", "x")
ALL = ("z_high", "z_low", "core", "y", "x")
PLANE = ("core", "y", "x")
HIGH = lax.Precision.HIGHEST
WHOLE = pl.BlockSpec(memory_space=pltpu.VMEM)
FAR = pl.BlockSpec(memory_space=pltpu.HBM)


def dot(left, right, dims=((1,), (0,))):
    return lax.dot_general(
        left, right, (dims, ((), ())), precision=HIGH, preferred_element_type=jnp.float32
    )


def upper_blocks(order):
    count = order // B
    return [(i, j) for i in range(count) for j in range(i, count)]


def packed_rows(order):
    count = order // B
    return count * (count - 1) // 2 * B + count // 2 * (B + B // 2)


def halves(value):
    top = value.astype(jnp.bfloat16)
    return top, (value - top.astype(jnp.float32)).astype(jnp.bfloat16)


def narrow_dot(left, right, dims=((1,), (0,))):
    return lax.dot_general(left, right, (dims, ((), ())), preferred_element_type=jnp.float32)


def gram_kernel(count_ref, rows, packed_ref, left_sum, right_sum):
    capacity, order = rows.shape
    height = capacity // CHUNKS
    wide = order // 2

    left_sum[...] = jnp.zeros_like(left_sum)
    right_sum[...] = jnp.zeros_like(right_sum)
    row = lax.broadcasted_iota(jnp.int32, (height, order), 0)

    @pl.loop(0, CHUNKS)
    def _(c):
        held = rows[pl.ds(pl.multiple_of(c * height, height), height), :]
        live = jnp.where(row < count_ref[0] - c * height, held, 0.0)
        top, low = halves(live)
        top_t, low_t = halves(live.T)
        for total, side in ((left_sum, slice(0, wide)), (right_sum, slice(wide, order))):
            tall = total.shape[0]
            term = narrow_dot(top_t[:tall], top[:, side])
            term += narrow_dot(low_t[:tall], top[:, side])
            term += narrow_dot(top_t[:tall], low[:, side])
            term += narrow_dot(low_t[:tall], low[:, side])
            total[...] += term

    def block(i, j):
        side, inner = divmod(j * B, wide)
        total = (left_sum, right_sum)[side]
        return total[i * B : (i + 1) * B, inner : inner + B]

    at = 0
    for i, j in upper_blocks(order):
        if i != j:
            packed_ref[at : at + B, :] = block(i, j)
            at += B
    half = B // 2
    lane = lax.broadcasted_iota(jnp.int32, (half, B), 1)
    for i in range(0, order // B, 2):
        first, second = block(i, i), block(i + 1, i + 1)
        packed_ref[at : at + half, :] = first[:half]
        packed_ref[at + half : at + B, :] = second[:half]
        packed_ref[at + B : at + B + half, :] = jnp.where(
            lane < half, pltpu.roll(first[half:], half, 1), second[half:]
        )
        at += B + half


def gram_of(rows_in, count):
    capacity, order = rows_in.shape
    return pl.pallas_call(
        gram_kernel,
        out_shape=jax.ShapeDtypeStruct((packed_rows(order), B), jnp.float32),
        in_specs=[pl.BlockSpec(memory_space=pltpu.SMEM), WHOLE],
        out_specs=WHOLE,
        scratch_shapes=[
            pltpu.VMEM((order // 2, order // 2), jnp.float32),
            pltpu.VMEM((order, order // 2), jnp.float32),
        ],
        compiler_params=pltpu.CompilerParams(vmem_limit_bytes=ROOM),
        name="gram",
    )(count, rows_in)


def spread(row):
    return jnp.broadcast_to(row, (SUB, row.shape[1]))


def thirds(value):
    top = value.astype(jnp.bfloat16)
    rest = value - top.astype(jnp.float32)
    middle = rest.astype(jnp.bfloat16)
    return top, middle, (rest - middle.astype(jnp.float32)).astype(jnp.bfloat16)


def stacked(value, order, axis):
    parts = thirds(value)
    return jnp.concatenate([parts[k] for k in order], axis=axis)


def exact_dot(left, right):
    return narrow_dot(stacked(left, LEFT, 1), stacked(right, RIGHT, 0))


def eliminate(strip, at):
    groups = NB // SUB
    lane = lax.broadcasted_iota(jnp.int32, (SUB, B), 1)
    sub = lax.broadcasted_iota(jnp.int32, (SUB, B), 0)
    rows = [strip[v * SUB : (v + 1) * SUB] for v in range(groups)]
    cols = [
        [
            None
            if v < j // SUB
            else jnp.broadcast_to(rows[v][:, at + j : at + j + 1], (SUB, B))
            for v in range(groups)
        ]
        for j in range(NB)
    ]
    diagonal = (lane >= at) & (lane < at + NB)
    rows = [
        jnp.where(diagonal, (lane == sub + (at + v * SUB)).astype(jnp.float32), rows[v])
        for v in range(groups)
    ]
    done = list(rows)
    pivot = spread(cols[0][0][:1])
    for j in range(NB):
        first, r = divmod(j, SUB)
        root = lax.rsqrt(pivot)
        if j + 1 < NB:
            g, q = divmod(j + 1, SUB)
            ahead = spread(cols[j][g][q : q + 1])
            pivot = spread(cols[j + 1][g][q : q + 1]) - ahead * ahead * (1.0 / pivot)
        scaled = [None if c is None else c * root for c in cols[j]]
        row = spread(rows[first][r : r + 1]) * root
        done[first] = jnp.where(sub == r, row, done[first])
        for l in range(j + 1, NB):
            g, q = divmod(l, SUB)
            factor = spread(scaled[g][q : q + 1])
            for v in range(g, groups):
                cols[l][v] = cols[l][v] - scaled[v] * factor
        for v in range(first, groups):
            rows[v] = rows[v] - scaled[v] * row
        cols[j] = None
    return jnp.concatenate(done)


def factor_block(block):
    strips = [block[b * NB : (b + 1) * NB] for b in range(B // NB)]
    lane = lax.broadcasted_iota(jnp.int32, (NB, B), 1)
    sub = lax.broadcasted_iota(jnp.int32, (NB, B), 0)
    inverse = []
    for b in range(B // NB):
        at = b * NB
        done = eliminate(strips[b], at)
        inverse.append(jnp.where(lane <= sub + at, done, 0.0))
        if at + NB < B:
            across = stacked(done, LEFT_WIDE, 0).T
            down = stacked(done, RIGHT_WIDE, 0)
            hit = (lane >= at) & (lane < at + NB)
            near = narrow_dot(across[at + NB : at + 2 * NB], down)
            strips[b + 1] = jnp.where(hit, 0.0, strips[b + 1]) - near
            if at + 2 * NB < B:
                rest = narrow_dot(across[at + 2 * NB :], down)
                for i in range(b + 2, B // NB):
                    o = (i - b - 2) * NB
                    strips[i] = jnp.where(hit, 0.0, strips[i]) - rest[o : o + NB]
    return jnp.concatenate(inverse)


def factor(scale, packed_ref, upper_ref, top_ref, low_ref, work):
    order = work.shape[0]
    at = 0
    for i, j in upper_blocks(order):
        if i != j:
            work[i * B : (i + 1) * B, j * B : (j + 1) * B] = packed_ref[at : at + B, :] * scale
            at += B
    half = B // 2
    right = lax.broadcasted_iota(jnp.int32, (half, B), 1) >= half
    for i in range(0, order // B, 2):
        both = packed_ref[at + B : at + B + half, :] * scale
        for k, low in ((0, pltpu.roll(both, half, 1)), (1, both)):
            lo = (i + k) * B
            span = slice(lo, lo + B)
            work[lo : lo + half, span] = packed_ref[at + k * half : at + (k + 1) * half, :] * scale
            work[lo + half : lo + B, span] = jnp.where(right, low, 0.0)
        at += B + half
    lane = lax.broadcasted_iota(jnp.int32, (B, B), 1)
    sub = lax.broadcasted_iota(jnp.int32, (B, B), 0)
    for s in range(order // B):
        lo, hi = s * B, (s + 1) * B
        here = slice(lo, hi)
        inverse = factor_block(work[here, here])
        across = stacked(inverse, LEFT, 1)
        if hi < order:
            near = slice(hi, hi + B)
            right = narrow_dot(across, stacked(work[here, near], RIGHT, 0))
            work[near, near] = work[near, near] - exact_dot(right.T, right)
            rights = [right]
            if hi + B < order:
                far = narrow_dot(across, stacked(work[here, hi + B :], RIGHT, 0))
                rights += [far[:, c : c + B] for c in range(0, far.shape[1], B)]
            for c, right in enumerate(rights):
                upper_ref[here, hi + c * B : hi + (c + 1) * B] = right
        own = narrow_dot(across, stacked(work[here, here], RIGHT, 0))
        upper_ref[here, here] = jnp.where(lane >= sub, own, 0.0)
        lefts = [inverse]
        if lo:
            left = narrow_dot(across, stacked(work[here, :lo], RIGHT, 0))
            upper_ref[here, :lo] = jnp.zeros((B, lo), jnp.float32)
            lefts = [left, inverse]
        lefts = jnp.concatenate(lefts, axis=1)
        top_ref[here, :hi], low_ref[here, :hi] = halves(lefts)
        if s % 2 == 0 and hi < order:
            top_ref[here, hi : hi + B] = jnp.zeros((B, B), jnp.bfloat16)
            low_ref[here, hi : hi + B] = jnp.zeros((B, B), jnp.bfloat16)
        if hi < order:
            turned = [stacked(right.T, LEFT, 1) for right in rights]
            change = narrow_dot(jnp.concatenate(turned), stacked(lefts, RIGHT, 0))
            if lo:
                work[hi:, :lo] = work[hi:, :lo] - change[:, :lo]
            work[hi:, here] = -change[:, lo:]
            for c in range(1, len(rights)):
                span = slice(hi + c * B, hi + (c + 1) * B)
                change = narrow_dot(
                    jnp.concatenate(turned[: c + 1]), stacked(rights[c], RIGHT, 0)
                )
                work[hi : hi + (c + 1) * B, span] = work[hi : hi + (c + 1) * B, span] - change


def solve_kernel(
    scale, scalars_ref, packed_ref, rows_ref, out_ref, share_ref,
    work, upper, top, low, result, sems,
):
    capacity, order = rows_ref.shape
    height = capacity // CHUNKS
    half = order // 2
    factor(scale, packed_ref, upper, top, low, work)
    share = share_ref.shape[0]
    share_ref[...] = upper[pl.ds(pl.multiple_of(scalars_ref[1] * share, share), share), :]
    row = lax.broadcasted_iota(jnp.int32, (height, order), 0)

    def store(c):
        span = pl.ds(pl.multiple_of(c * height, height), height)
        return pltpu.make_async_copy(result.at[span], out_ref.at[span], sems.at[c])

    @pl.loop(0, CHUNKS)
    def _(c):
        span = pl.ds(pl.multiple_of(c * height, height), height)
        live = jnp.where(row < scalars_ref[0] - c * height, rows_ref[span, :], 0.0)
        live_top, live_low = halves(live)
        for k in range(2):
            lo, hi = k * half, (k + 1) * half
            value = narrow_dot(live_top[:, :hi], top[lo:hi, :hi], ((1,), (1,)))
            value += narrow_dot(live_low[:, :hi], top[lo:hi, :hi], ((1,), (1,)))
            value += narrow_dot(live_top[:, :hi], low[lo:hi, :hi], ((1,), (1,)))
            result[span, lo:hi] = value
        store(c).start()

    for c in range(CHUNKS):
        store(c).wait()


def solved(packed, rows_in, scalars, members, scale):
    capacity, order = rows_in.shape
    square = pltpu.VMEM((order, order), jnp.float32)
    tall = pltpu.VMEM((capacity, order), jnp.float32)
    return pl.pallas_call(
        functools.partial(solve_kernel, scale),
        out_shape=[
            jax.ShapeDtypeStruct(rows_in.shape, jnp.float32),
            jax.ShapeDtypeStruct((order // members, order), jnp.float32),
        ],
        in_specs=[pl.BlockSpec(memory_space=pltpu.SMEM), WHOLE, WHOLE],
        out_specs=[FAR, WHOLE],
        scratch_shapes=[
            square,
            square,
            pltpu.VMEM((order, order), jnp.bfloat16),
            pltpu.VMEM((order, order), jnp.bfloat16),
            tall,
            pltpu.SemaphoreType.DMA((CHUNKS,)),
        ],
        compiler_params=pltpu.CompilerParams(vmem_limit_bytes=ROOM),
        name="solve",
    )(scalars, packed, rows_in)


def exchanged(tiles, axis):
    return lax.all_to_all(tiles, axis, split_axis=0, concat_axis=0, tiled=True)


def everyone(value, axis):
    return exchanged(jnp.broadcast_to(value, (lax.axis_size(axis), *value.shape)), axis)


def summed(packed):
    tiles = packed.reshape(lax.axis_size(PLANE), -1, SUB // 2, B)
    own = exchanged(tiles, PLANE).sum(axis=0)
    own = everyone(own, "z_low").sum(axis=0)
    own = everyone(own, "z_high").sum(axis=0)
    return everyone(own, PLANE).reshape(-1, B)


def shards(sketch, row_counts):
    capacity, order = sketch.shape
    members = lax.axis_size(DEV)
    row_total = lax.axis_size(ALL) * HOLD * (capacity // SLOTS)
    scalars = jnp.stack([row_counts[0], lax.axis_index(DEV)])
    packed = summed(gram_of(sketch, scalars))
    return solved(packed, sketch, scalars, members, 1.0 / row_total)


def solution(mesh):
    finer = Mesh(mesh.devices.reshape(4, 4, 2, 4, 4), ALL)
    return jax.shard_map(
        shards,
        mesh=finer,
        in_specs=(P(ALL, None), P(ALL)),
        out_specs=(P(ALL, None), P(DEV, None)),
        check_vma=False,
    )
```

```python
import functools

import jax
import jax.numpy as jnp
from jax import lax
from jax.experimental import pallas as pl
from jax.experimental.pallas import tpu as pltpu
from jax.sharding import Mesh
from jax.sharding import PartitionSpec as P

SLOTS = 16
HOLD = 4
B = 128
NB = 32
SUB = 8
CHUNKS = 4
ROOM = 24 * 1024 * 1024
LEFT, RIGHT = (2, 1, 0, 1, 0, 0), (0, 1, 2, 0, 1, 0)
LEFT_WIDE, RIGHT_WIDE = (2, 1, *LEFT), (1, 2, *RIGHT)
DEV = ("y", "x")
ALL = ("z_high", "z_low", "core", "y", "x")
PLANE = ("core", "y", "x")
HIGH = lax.Precision.HIGHEST
WHOLE = pl.BlockSpec(memory_space=pltpu.VMEM)
FAR = pl.BlockSpec(memory_space=pltpu.HBM)


def dot(left, right, dims=((1,), (0,))):
    return lax.dot_general(
        left, right, (dims, ((), ())), precision=HIGH, preferred_element_type=jnp.float32
    )


def upper_blocks(order):
    count = order // B
    return [(i, j) for i in range(count) for j in range(i, count)]


def packed_rows(order):
    count = order // B
    return count * (count - 1) // 2 * B + count // 2 * (B + B // 2)


def halves(value):
    top = value.astype(jnp.bfloat16)
    return top, (value - top.astype(jnp.float32)).astype(jnp.bfloat16)


def narrow_dot(left, right, dims=((1,), (0,))):
    return lax.dot_general(left, right, (dims, ((), ())), preferred_element_type=jnp.float32)


def gram_kernel(_, top_ref, low_ref, packed_ref, left_sum, right_sum):
    order = top_ref.shape[1]
    wide = order // 2
    top, low = top_ref[...], low_ref[...]
    top_t, low_t = top.T, low.T
    for total, side in ((left_sum, slice(0, wide)), (right_sum, slice(wide, order))):
        tall = total.shape[0]
        term = narrow_dot(top_t[:tall], top[:, side])
        term += narrow_dot(low_t[:tall], top[:, side])
        term += narrow_dot(top_t[:tall], low[:, side])
        term += narrow_dot(low_t[:tall], low[:, side])
        total[...] = term

    def block(i, j):
        side, inner = divmod(j * B, wide)
        total = (left_sum, right_sum)[side]
        return total[i * B : (i + 1) * B, inner : inner + B]

    at = 0
    for i, j in upper_blocks(order):
        if i != j:
            packed_ref[at : at + B, :] = block(i, j)
            at += B
    half = B // 2
    lane = lax.broadcasted_iota(jnp.int32, (half, B), 1)
    for i in range(0, order // B, 2):
        first, second = block(i, i), block(i + 1, i + 1)
        packed_ref[at : at + half, :] = first[:half]
        packed_ref[at + half : at + B, :] = second[:half]
        packed_ref[at + B : at + B + half, :] = jnp.where(
            lane < half, pltpu.roll(first[half:], half, 1), second[half:]
        )
        at += B + half


def live_halves(rows_in, count):
    row = lax.broadcasted_iota(jnp.int32, rows_in.shape, 0)
    live = jnp.where(row < count, rows_in, 0.0)
    rounded = lax.reduce_precision(live, 8, 7)
    return rounded.astype(jnp.bfloat16), (live - rounded).astype(jnp.bfloat16)


def gram_of(index, live_top, live_low):
    order = live_top.shape[1]
    return pl.pallas_call(
        gram_kernel,
        out_shape=jax.ShapeDtypeStruct((packed_rows(order), B), jnp.float32),
        in_specs=[pl.BlockSpec(memory_space=pltpu.SMEM), WHOLE, WHOLE],
        out_specs=WHOLE,
        scratch_shapes=[
            pltpu.VMEM((order // 2, order // 2), jnp.float32),
            pltpu.VMEM((order, order // 2), jnp.float32),
        ],
        compiler_params=pltpu.CompilerParams(vmem_limit_bytes=ROOM),
        name="gram",
    )(index, live_top, live_low)


def spread(row):
    return jnp.broadcast_to(row, (SUB, row.shape[1]))


def thirds(value):
    top = value.astype(jnp.bfloat16)
    rest = value - top.astype(jnp.float32)
    middle = rest.astype(jnp.bfloat16)
    return top, middle, (rest - middle.astype(jnp.float32)).astype(jnp.bfloat16)


def stacked(value, order, axis):
    parts = thirds(value)
    return jnp.concatenate([parts[k] for k in order], axis=axis)


def exact_dot(left, right):
    return narrow_dot(stacked(left, LEFT, 1), stacked(right, RIGHT, 0))


def eliminate(strip, at):
    groups = NB // SUB
    lane = lax.broadcasted_iota(jnp.int32, (SUB, B), 1)
    sub = lax.broadcasted_iota(jnp.int32, (SUB, B), 0)
    rows = [strip[v * SUB : (v + 1) * SUB] for v in range(groups)]
    cols = [
        [
            None
            if v < j // SUB
            else jnp.broadcast_to(rows[v][:, at + j : at + j + 1], (SUB, B))
            for v in range(groups)
        ]
        for j in range(NB)
    ]
    diagonal = (lane >= at) & (lane < at + NB)
    rows = [
        jnp.where(diagonal, (lane == sub + (at + v * SUB)).astype(jnp.float32), rows[v])
        for v in range(groups)
    ]
    done = list(rows)
    pivot = spread(cols[0][0][:1])
    for j in range(NB):
        first, r = divmod(j, SUB)
        root = lax.rsqrt(pivot)
        if j + 1 < NB:
            g, q = divmod(j + 1, SUB)
            ahead = spread(cols[j][g][q : q + 1])
            pivot = spread(cols[j + 1][g][q : q + 1]) - ahead * ahead * (1.0 / pivot)
        scaled = [None if c is None else c * root for c in cols[j]]
        row = spread(rows[first][r : r + 1]) * root
        done[first] = jnp.where(sub == r, row, done[first])
        for l in range(j + 1, NB):
            g, q = divmod(l, SUB)
            factor = spread(scaled[g][q : q + 1])
            for v in range(g, groups):
                cols[l][v] = cols[l][v] - scaled[v] * factor
        for v in range(first, groups):
            rows[v] = rows[v] - scaled[v] * row
        cols[j] = None
    return jnp.concatenate(done)


def factor_block(block):
    strips = [block[b * NB : (b + 1) * NB] for b in range(B // NB)]
    lane = lax.broadcasted_iota(jnp.int32, (NB, B), 1)
    sub = lax.broadcasted_iota(jnp.int32, (NB, B), 0)
    inverse = []
    for b in range(B // NB):
        at = b * NB
        done = eliminate(strips[b], at)
        inverse.append(jnp.where(lane <= sub + at, done, 0.0))
        if at + NB < B:
            across = stacked(done, LEFT_WIDE, 0).T
            down = stacked(done, RIGHT_WIDE, 0)
            hit = (lane >= at) & (lane < at + NB)
            near = narrow_dot(across[at + NB : at + 2 * NB], down)
            strips[b + 1] = jnp.where(hit, 0.0, strips[b + 1]) - near
            if at + 2 * NB < B:
                rest = narrow_dot(across[at + 2 * NB :], down)
                for i in range(b + 2, B // NB):
                    o = (i - b - 2) * NB
                    strips[i] = jnp.where(hit, 0.0, strips[i]) - rest[o : o + NB]
    return jnp.concatenate(inverse)


def factor(scale, packed_ref, upper_ref, top_ref, low_ref, work):
    order = work.shape[0]
    at = 0
    for i, j in upper_blocks(order):
        if i != j:
            work[i * B : (i + 1) * B, j * B : (j + 1) * B] = packed_ref[at : at + B, :] * scale
            at += B
    half = B // 2
    right = lax.broadcasted_iota(jnp.int32, (half, B), 1) >= half
    for i in range(0, order // B, 2):
        both = packed_ref[at + B : at + B + half, :] * scale
        for k, low in ((0, pltpu.roll(both, half, 1)), (1, both)):
            lo = (i + k) * B
            span = slice(lo, lo + B)
            work[lo : lo + half, span] = packed_ref[at + k * half : at + (k + 1) * half, :] * scale
            work[lo + half : lo + B, span] = jnp.where(right, low, 0.0)
        at += B + half
    lane = lax.broadcasted_iota(jnp.int32, (B, B), 1)
    sub = lax.broadcasted_iota(jnp.int32, (B, B), 0)
    for s in range(order // B):
        lo, hi = s * B, (s + 1) * B
        here = slice(lo, hi)
        inverse = factor_block(work[here, here])
        across = stacked(inverse, LEFT, 1)
        if hi < order:
            near = slice(hi, hi + B)
            right = narrow_dot(across, stacked(work[here, near], RIGHT, 0))
            work[near, near] = work[near, near] - exact_dot(right.T, right)
            rights = [right]
            if hi + B < order:
                far = narrow_dot(across, stacked(work[here, hi + B :], RIGHT, 0))
                rights += [far[:, c : c + B] for c in range(0, far.shape[1], B)]
            for c, right in enumerate(rights):
                upper_ref[here, hi + c * B : hi + (c + 1) * B] = right
        own = narrow_dot(across, stacked(work[here, here], RIGHT, 0))
        upper_ref[here, here] = jnp.where(lane >= sub, own, 0.0)
        lefts = [inverse]
        if lo:
            left = narrow_dot(across, stacked(work[here, :lo], RIGHT, 0))
            upper_ref[here, :lo] = jnp.zeros((B, lo), jnp.float32)
            lefts = [left, inverse]
        lefts = jnp.concatenate(lefts, axis=1)
        top_ref[here, :hi], low_ref[here, :hi] = halves(lefts)
        if s % 2 == 0 and hi < order:
            top_ref[here, hi : hi + B] = jnp.zeros((B, B), jnp.bfloat16)
            low_ref[here, hi : hi + B] = jnp.zeros((B, B), jnp.bfloat16)
        if hi < order:
            turned = [stacked(right.T, LEFT, 1) for right in rights]
            change = narrow_dot(jnp.concatenate(turned), stacked(lefts, RIGHT, 0))
            if lo:
                work[hi:, :lo] = work[hi:, :lo] - change[:, :lo]
            work[hi:, here] = -change[:, lo:]
            for c in range(1, len(rights)):
                span = slice(hi + c * B, hi + (c + 1) * B)
                change = narrow_dot(
                    jnp.concatenate(turned[: c + 1]), stacked(rights[c], RIGHT, 0)
                )
                work[hi : hi + (c + 1) * B, span] = work[hi : hi + (c + 1) * B, span] - change


def solve_kernel(
    scale, index_ref, packed_ref, live_top_ref, live_low_ref, out_ref, share_ref,
    work, upper, top, low, result, sems,
):
    capacity, order = live_top_ref.shape
    height = capacity // CHUNKS
    half = order // 2
    factor(scale, packed_ref, upper, top, low, work)
    share = share_ref.shape[0]
    share_ref[...] = upper[pl.ds(pl.multiple_of(index_ref[0] * share, share), share), :]

    def store(c):
        span = pl.ds(pl.multiple_of(c * height, height), height)
        return pltpu.make_async_copy(result.at[span], out_ref.at[span], sems.at[c])

    @pl.loop(0, CHUNKS)
    def _(c):
        span = pl.ds(pl.multiple_of(c * height, height), height)
        live_top, live_low = live_top_ref[span, :], live_low_ref[span, :]
        for k in range(2):
            lo, hi = k * half, (k + 1) * half
            value = narrow_dot(live_top[:, :hi], top[lo:hi, :hi], ((1,), (1,)))
            value += narrow_dot(live_low[:, :hi], top[lo:hi, :hi], ((1,), (1,)))
            value += narrow_dot(live_top[:, :hi], low[lo:hi, :hi], ((1,), (1,)))
            result[span, lo:hi] = value
        store(c).start()

    for c in range(CHUNKS):
        store(c).wait()


def solved(packed, live_top, live_low, index, members, scale):
    capacity, order = live_top.shape
    square = pltpu.VMEM((order, order), jnp.float32)
    tall = pltpu.VMEM((capacity, order), jnp.float32)
    return pl.pallas_call(
        functools.partial(solve_kernel, scale),
        out_shape=[
            jax.ShapeDtypeStruct((capacity, order), jnp.float32),
            jax.ShapeDtypeStruct((order // members, order), jnp.float32),
        ],
        in_specs=[pl.BlockSpec(memory_space=pltpu.SMEM), WHOLE, WHOLE, WHOLE],
        out_specs=[FAR, WHOLE],
        scratch_shapes=[
            square,
            square,
            pltpu.VMEM((order, order), jnp.bfloat16),
            pltpu.VMEM((order, order), jnp.bfloat16),
            tall,
            pltpu.SemaphoreType.DMA((CHUNKS,)),
        ],
        compiler_params=pltpu.CompilerParams(vmem_limit_bytes=ROOM),
        name="solve",
    )(index, packed, live_top, live_low)


def exchanged(tiles, axis):
    return lax.all_to_all(tiles, axis, split_axis=0, concat_axis=0, tiled=True)


def everyone(value, axis):
    return exchanged(jnp.broadcast_to(value, (lax.axis_size(axis), *value.shape)), axis)


def summed(packed):
    tiles = packed.reshape(lax.axis_size(PLANE), -1, SUB // 2, B)
    own = exchanged(tiles, PLANE).sum(axis=0)
    own = everyone(own, "z_low").sum(axis=0)
    own = everyone(own, "z_high").sum(axis=0)
    return everyone(own, PLANE).reshape(-1, B)


def shards(sketch, row_counts):
    capacity, order = sketch.shape
    members = lax.axis_size(DEV)
    row_total = lax.axis_size(ALL) * HOLD * (capacity // SLOTS)
    index = lax.axis_index(DEV).reshape(1)
    live_top, live_low = live_halves(sketch, row_counts[0])
    packed = summed(gram_of(index, live_top, live_low))
    return solved(packed, live_top, live_low, index, members, 1.0 / row_total)


def solution(mesh):
    finer = Mesh(mesh.devices.reshape(4, 4, 2, 4, 4), ALL)
    return jax.shard_map(
        shards,
        mesh=finer,
        in_specs=(P(ALL, None), P(ALL)),
        out_specs=(P(ALL, None), P(DEV, None)),
        check_vma=False,
    )
```
